32 devices in a mesh: freq: 4 (over y, core), stn: 8 (over z, x).
Axes of the slice: x: 2, y: 2, z: 4, core: 2. Of those that a mesh axis runs over, the one named last changes fastest.
Arguments:
- samples: bfloat16 [4, 256, 24, 2, 128], P('freq', 'stn'), may hold values from -8 to 8, as said below
- window: float32 [128], replicated, may hold values from 0.1 to 1
- group_of_device: int32 [8], replicated, may hold values from 0 to 7, each once
- owner_map: int32 [8, 8], replicated, may hold values from 0 to 7, as said below
Outputs:
- owned: bfloat16 [2, 32, 8, 8, 1024], P(None, None, 'stn', 'freq')
The draws below stay inside these ranges and needn't reach their ends.
Inputs may be any that keep to these rules, and one draw needn't show every extreme that they name: `samples`: samples are finite and bounded. Every row and every column of owner_map names each stn index exactly once.
All inputs are finite; a program needn't handle non-finite values.
Results may differ from the reference program's by a relative error of at most 0.0065.
Values may be sent and summed in bfloat16 or wider, within the bound.
A program may use at most 64 MiB of HBM per device.

```python
import math
import jax
import jax.numpy as jnp
from jax import lax

FFT_LEN = 128
AVG = 16
SPEC = 24
GRP_IN = 32
CH_OUT = 8
GROUPS = 8
BANDS = 4
INPUTS = 256
CHANNELS = 32


def draw_samples(key, part):
    sky_sources = 32
    keys = jax.random.split(key, 3)
    shape = (BANDS, INPUTS, SPEC, 2, FFT_LEN)
    gains = jax.random.normal(keys[1], (INPUTS, sky_sources), jnp.float32)
    signals = jax.random.normal(keys[2], (BANDS, sky_sources, SPEC, 2, FFT_LEN), jnp.float32)
    common = jnp.einsum('ik,bktrn->bitrn', gains, signals) / math.sqrt(sky_sources)
    noise = jax.random.normal(keys[0], shape, jnp.float32)
    total = 0.55 * noise + common
    return jnp.clip(total, -8.0, 8.0).astype(jnp.bfloat16)


def draw_owner_map(key, part):
    keys = jax.random.split(key, 3)
    row_shift = jax.random.permutation(keys[0], GROUPS)
    col_shift = jax.random.permutation(keys[1], GROUPS)
    labels = jax.random.permutation(keys[2], GROUPS)
    return labels[(row_shift[:, None] + col_shift[None, :]) % GROUPS].astype(jnp.int32)


def setup_inputs(seed: int = 0) -> dict:
    key_of = jax.random.split(jax.random.key(seed), 5)
    return {
        "samples": draw_samples(jax.random.fold_in(key_of[4], 71), 0),
        "window": jnp.clip(jnp.exp(jax.random.uniform(key_of[1], (FFT_LEN,), jnp.float32, math.log(0.1), math.log(1.0))), 0.1, 1.0),
        "group_of_device": jax.random.permutation(key_of[2], GROUPS).astype(jnp.int32),
        "owner_map": draw_owner_map(jax.random.fold_in(key_of[4], 71), 0),
    }


def channel_matrix(window):
    length = window.shape[0]
    index = jnp.arange(length, dtype=jnp.int32)
    product = index[:, None] * index[None, :] % length
    theta = product.astype(jnp.float32) * (2.0 * math.pi / length)
    weights = window[:, None] / math.sqrt(length)
    cosine = weights * jnp.cos(theta)
    sine = weights * jnp.sin(theta)
    upper = jnp.concatenate([cosine, -sine], axis=1)
    lower = jnp.concatenate([sine, cosine], axis=1)
    return jnp.concatenate([upper, lower], axis=0)

def split_matrix(matrix):
    high = matrix.astype(jnp.bfloat16)
    low = (matrix - high.astype(jnp.float32)).astype(jnp.bfloat16)
    return (high, low)

def channelize(block, high, low):
    rows = block.shape[0]
    flat = block.reshape(rows * SPEC, 2 * FFT_LEN)
    spectra = jnp.dot(flat, high, preferred_element_type=jnp.float32) + jnp.dot(flat, low, preferred_element_type=jnp.float32)
    spectra = spectra.astype(jnp.bfloat16).reshape(rows, SPEC, 2, CH_OUT, AVG)
    return spectra.transpose(3, 0, 2, 1, 4).reshape(CH_OUT, rows, 2 * SPEC * AVG)

def reference(samples, window, group_of_device, owner_map):
    high, low = split_matrix(channel_matrix(window))
    order = jnp.arange(GROUPS, dtype=jnp.int32)
    dev_of_group = jnp.zeros((GROUPS,), jnp.int32).at[group_of_device].set(order)
    grouped = samples.reshape(BANDS, GROUPS, GRP_IN, SPEC, 2, FFT_LEN)
    grouped = jnp.take(grouped, dev_of_group, axis=1).reshape(BANDS, INPUTS, SPEC, 2, FFT_LEN)
    column_for = jnp.zeros((GROUPS, GROUPS), jnp.int32).at[order[:, None], owner_map].set(jnp.broadcast_to(order[None, :], (GROUPS, GROUPS)))

    def one_band(band):
        spectra = channelize(band, high, low).astype(jnp.float32)
        half = spectra.shape[2] // 2
        swapped = jnp.concatenate([spectra[..., half:], -spectra[..., :half]], axis=-1)
        stacked = jnp.stack([spectra, swapped])
        vis = jnp.einsum('pcak,cbk->pcab', stacked, spectra)
        vis = (vis * (1.0 / (AVG * SPEC))).astype(jnp.bfloat16)
        vis = vis.reshape(2, CH_OUT, GROUPS, GRP_IN, GROUPS, GRP_IN).transpose(0, 1, 2, 4, 3, 5)
        vis = vis.reshape(2, CH_OUT, GROUPS, GROUPS, GRP_IN * GRP_IN)
        picked = jnp.take_along_axis(vis, column_for[None, None, :, :, None], axis=3)
        return picked.transpose(0, 1, 3, 2, 4)
    result = lax.map(one_band, grouped)
    result = result.transpose(1, 0, 2, 3, 4, 5)
    return result.reshape(2, CHANNELS, GROUPS, GROUPS, GRP_IN * GRP_IN)
```

```python
import functools
import math

import jax
import jax.numpy as jnp
import numpy as np
from jax import lax
from jax.experimental import pallas as pl
from jax.experimental.pallas import tpu as pltpu
from jax.sharding import PartitionSpec as P

AVG = 16
LANES = 128
MESH = pl.DeviceIdType.MESH
OUT_SPACE = pltpu.VMEM


def swap_blocks(blocks, width):
    blocks = list(blocks)
    count = len(blocks)
    lane = lax.broadcasted_iota(jnp.int32, blocks[0].shape, 1) // width
    step = count // 2
    while step:
        upper = (lane // step) % 2 == 1
        for i in range(count):
            if (i // step) % 2 == 0:
                u, v = blocks[i], blocks[i + step]
                shift = step * width
                blocks[i] = jnp.where(upper, pltpu.roll(v, shift, 1), u)
                blocks[i + step] = jnp.where(upper, v, pltpu.roll(u, LANES - shift, 1))
        step //= 2
    return blocks


def kernel(
    nf, ns, rows, spec,
    x_hbm, w_hbm, trig_hbm, god_hbm, own_hbm,
    out_ref,
    x_ref, w_ref, trig_ref, god_ref, own_ref,
    xf, send1, held, left, vis, tiles, mixed, send2, dev_of, table,
    lsem, row_sem, ssem1, rsem1, ssem2, rsem2,
):
    length = LANES
    ch_out = length // AVG
    spread = ns // ch_out
    rpf = ns // nf
    fl_count = ch_out // rpf
    chunks = spec // ch_out
    step = 2 * ch_out
    b = lax.axis_index("freq")
    me = lax.axis_index("stn")

    def load(n, src, dst):
        return pltpu.make_async_copy(src, dst, lsem.at[n])

    def load_x(th):
        return load(4 + th, x_hbm.at[:, th * step : (th + 1) * step, :], x_ref.at[th])

    load_w = load(0, w_hbm, w_ref)
    load_trig = load(1, trig_hbm, trig_ref)
    load_god = load(2, god_hbm, god_ref)
    load_own = load(3, own_hbm, own_ref)
    load_w.start()
    load_trig.start()
    for th in range(chunks):
        load_x(th).start()
    load_god.start()
    load_own.start()

    barrier = pltpu.get_barrier_semaphore()
    offsets = sorted(range(1, ns), key=lambda o: abs(o - ns / 2))
    for off in offsets:
        pl.semaphore_signal(
            barrier, inc=1, device_id=(b, lax.rem(me + off, ns)), device_id_type=MESH
        )
    for off in range(1, nf):
        pl.semaphore_signal(
            barrier, inc=1, device_id=(lax.rem(b + off, nf), me), device_id_type=MESH
        )

    load_w.wait()
    load_trig.wait()
    weights = jnp.broadcast_to(w_ref[...], (length, length)).T * (1.0 / math.sqrt(length))
    cosine = weights * trig_ref[0]
    sine = weights * trig_ref[1]
    matrix = jnp.concatenate(
        [jnp.concatenate([cosine, -sine], axis=1), jnp.concatenate([sine, cosine], axis=1)], axis=0
    )
    high = matrix.astype(jnp.bfloat16)
    low = (matrix - high.astype(jnp.float32)).astype(jnp.bfloat16)

    for th in range(chunks):
        load_x(th).wait()
    for th in range(chunks):
        xf[th] = x_ref[th].astype(jnp.float32).reshape(rows * step, length)
    for th in range(chunks):
        parts = []
        for t in range(ch_out):
            re = xf[th, pl.ds(2 * t, rows, stride=step), :]
            im = xf[th, pl.ds(2 * t + 1, rows, stride=step), :]
            parts.append(jnp.concatenate([re, im], axis=1).astype(jnp.bfloat16))
        flat = jnp.concatenate(parts, axis=0)
        spectra = jnp.dot(flat, high, preferred_element_type=jnp.float32) + jnp.dot(
            flat, low, preferred_element_type=jnp.float32
        )
        for p in range(2):
            blocks = [
                spectra[i * rows : (i + 1) * rows, p * LANES : (p + 1) * LANES]
                for i in range(ch_out)
            ]
            blocks = swap_blocks(blocks, AVG)
            for k in range(ch_out):
                send1[k, th, :, p * LANES : (p + 1) * LANES] = blocks[k].astype(jnp.bfloat16)

    def first_copy(d, mine):
        return pltpu.make_async_remote_copy(
            src_ref=send1.at[d // spread],
            dst_ref=held.at[mine],
            send_sem=ssem1.at[d],
            recv_sem=rsem1.at[mine],
            device_id=(b, d),
            device_id_type=MESH,
        )

    pl.semaphore_wait(barrier, ns - 1 + nf - 1)
    for off in offsets:
        first_copy(lax.rem(me + off, ns), me).start()

    for off in range(1, nf):
        pl.semaphore_signal(
            row_sem, inc=1, device_id=(lax.rem(b + off, nf), me), device_id_type=MESH
        )
    held[me] = send1[me // spread]

    load_god.wait()
    load_own.wait()

    def find_dev(g, carry):
        def body(s, acc):
            return jnp.where(god_ref[s] == g, s, acc)

        dev_of[g] = lax.fori_loop(0, ns, body, jnp.int32(0), unroll=min(ns, 8))
        return carry

    lax.fori_loop(0, ns, find_dev, 0)
    quarter = lax.rem(me, spread)

    def find_col(i, carry):
        g1 = quarter * ch_out + i // ns
        o = lax.rem(i, ns)

        def body(g2, acc):
            return jnp.where(own_ref[g1, g2] == o, dev_of[g2], acc)

        table[i] = lax.fori_loop(0, ns, body, jnp.int32(0), unroll=min(ns, 8))
        return carry

    lax.fori_loop(0, ch_out * ns, find_col, 0)
    pl.semaphore_wait(row_sem, nf - 1)

    channel = b * ch_out + me // spread
    first_row = quarter * fl_count

    def second_copy(fl, o):
        return pltpu.make_async_remote_copy(
            src_ref=send2.at[fl * ns + o],
            dst_ref=out_ref.at[:, channel],
            send_sem=ssem2.at[fl * ns + o],
            recv_sem=rsem2.at[channel],
            device_id=(first_row + fl, o),
            device_id_type=MESH,
        )

    def unless_mine(fl, o, run):
        mine = jnp.logical_and(first_row + fl == b, o == me)
        pl.when(jnp.logical_not(mine))(run)

    per_tile = LANES // rows
    sub = rows // per_tile
    span = rpf * rows
    wide = min(2 * per_tile, ns)
    cols = wide * rows

    def wait_first(i, carry):
        first_copy(me, lax.rem(me + i, ns)).wait_recv()
        return carry

    lax.fori_loop(1, ns, wait_first, 0)

    for fl in range(fl_count):
        for g in range(rpf):
            x = held[dev_of[(first_row + fl) * rpf + g]]
            for th in range(chunks):
                left[th, g * rows : (g + 1) * rows, :] = x[th]
                left[th, span + g * rows : span + (g + 1) * rows, :LANES] = x[th, :, LANES:]
                left[th, span + g * rows : span + (g + 1) * rows, LANES:] = -x[th, :, :LANES]
        for c in range(ns // wide):
            block = sum(
                lax.dot_general(
                    left[th],
                    held[c * wide : (c + 1) * wide, th].reshape(cols, 2 * LANES),
                    (((1,), (1,)), ((), ())),
                    preferred_element_type=jnp.float32,
                )
                for th in range(chunks)
            ) * (1.0 / (AVG * spec))
            for h in range(cols // LANES):
                vis[h] = block[:, h * LANES : (h + 1) * LANES]
            for h in range(cols // LANES):
                blocks = [
                    vis[h, pl.ds(q, 2 * span // per_tile, stride=per_tile), :]
                    for q in range(per_tile)
                ]
                blocks = swap_blocks(blocks, rows)
                for s in range(per_tile):
                    tiles[c * wide + h * per_tile + s] = blocks[s].reshape(2 * rpf, sub, LANES)

        def build(o, carry):
            for g in range(rpf):
                source = table[(fl * rpf + g) * ns + o]
                for p in range(2):
                    mixed[o, p, pl.ds(g, sub, stride=rpf), :] = tiles[source, p * rpf + g]
            for p in range(2):
                for r in range(sub):
                    send2[fl * ns + o, p, :, r * LANES : (r + 1) * LANES] = mixed[
                        o, p, r * rpf : (r + 1) * rpf, :
                    ].astype(jnp.bfloat16)
            unless_mine(fl, o, lambda: second_copy(fl, o).start())
            return carry

        lax.fori_loop(0, ns, build, 0, unroll=min(ns, 8))

    own_here = quarter == b // fl_count

    @pl.when(own_here)
    def _():
        own = pltpu.make_async_copy(
            send2.at[lax.rem(b, fl_count) * ns + me], out_ref.at[:, channel], lsem.at[0]
        )
        own.start()
        own.wait()

    def wait_first_send(i, carry):
        first_copy(lax.rem(me + i, ns), me).wait_send()
        return carry

    lax.fori_loop(1, ns, wait_first_send, 0)

    def arrived(slot):
        pltpu.make_async_remote_copy(
            src_ref=send2.at[0],
            dst_ref=out_ref.at[:, slot],
            send_sem=ssem2.at[0],
            recv_sem=rsem2.at[slot],
            device_id=(b, me),
            device_id_type=MESH,
        ).wait_recv()

    def wait_arrival(i, carry):
        arrived(lax.rem(channel + i, nf * ch_out))
        return carry

    pl.when(jnp.logical_not(own_here))(lambda: arrived(channel))
    lax.fori_loop(1, nf * ch_out, wait_arrival, 0)

    def wait_second(i, carry):
        fl, o = i // ns, lax.rem(i, ns)
        unless_mine(fl, o, lambda: second_copy(fl, o).wait_send())
        return carry

    lax.fori_loop(0, fl_count * ns, wait_second, 0)


def shards(nf, ns, samples, window, group_of_device, owner_map):
    _, rows, spec, _, length = samples.shape
    ch_out = length // AVG
    rpf = ns // nf
    fl_count = ch_out // rpf
    per_tile = LANES // rows
    sub = rows // per_tile
    chunks = spec // ch_out
    index = np.arange(length)
    theta = (index[:, None] * index[None, :] % length) * (2.0 * math.pi / length)
    trig = jnp.asarray(np.stack([np.cos(theta), np.sin(theta)]), jnp.float32)
    x = samples.reshape(rows, spec * 2, length)
    hbm = pl.BlockSpec(memory_space=pltpu.HBM)
    out = pl.pallas_call(
        functools.partial(kernel, nf, ns, rows, spec),
        out_shape=pltpu.VMEM((2, nf * ch_out, rpf, sub * LANES), jnp.bfloat16),
        in_specs=[hbm] * 5,
        out_specs=pl.BlockSpec(memory_space=OUT_SPACE),
        scratch_shapes=[
            pltpu.VMEM((chunks, rows, 2 * ch_out, length), jnp.bfloat16),
            pltpu.VMEM((1, length), jnp.float32),
            pltpu.VMEM((2, length, length), jnp.float32),
            pltpu.SMEM((ns,), jnp.int32),
            pltpu.SMEM((ns, ns), jnp.int32),
            pltpu.VMEM((chunks, rows * 2 * ch_out, length), jnp.float32),
            pltpu.VMEM((ch_out, chunks, rows, 2 * LANES), jnp.bfloat16),
            pltpu.VMEM((ns, chunks, rows, 2 * LANES), jnp.bfloat16),
            pltpu.VMEM((chunks, 2 * rpf * rows, 2 * LANES), jnp.bfloat16),
            pltpu.VMEM((2, 2 * rpf * rows, LANES), jnp.float32),
            pltpu.VMEM((ns, 2 * rpf, sub, LANES), jnp.float32),
            pltpu.VMEM((ns, 2, sub * rpf, LANES), jnp.float32),
            pltpu.VMEM((fl_count * ns, 2, rpf, sub * LANES), jnp.bfloat16),
            pltpu.SMEM((ns,), jnp.int32),
            pltpu.SMEM((ch_out * ns,), jnp.int32),
            pltpu.SemaphoreType.DMA((4 + chunks,)),
            pltpu.SemaphoreType.REGULAR,
            pltpu.SemaphoreType.DMA((ns,)),
            pltpu.SemaphoreType.DMA((ns,)),
            pltpu.SemaphoreType.DMA((fl_count * ns,)),
            pltpu.SemaphoreType.DMA((nf * ch_out,)),
        ],
        compiler_params=pltpu.CompilerParams(
            collective_id=0, has_side_effects=True, vmem_limit_bytes=60 * 1024 * 1024
        ),
    )(x, window.reshape(1, length), trig, group_of_device, owner_map)
    return out[:, :, None]


def solution(mesh):
    return jax.shard_map(
        functools.partial(shards, mesh.shape["freq"], mesh.shape["stn"]),
        mesh=mesh,
        in_specs=(P("freq", "stn", None, None, None), P(), P(), P()),
        out_specs=P(None, None, "stn", "freq", None),
        check_vma=False,
    )
```

```python
import functools
import math

import jax
import jax.numpy as jnp
import numpy as np
from jax import lax
from jax.experimental import pallas as pl
from jax.experimental.pallas import tpu as pltpu
from jax.sharding import PartitionSpec as P

AVG = 16
LANES = 128
LEAD = 3
HOLD = 1
SLOW_EIGHTHS = (4, 3, 5, 2, 1, 6, 7)
FAST_EIGHTHS = (4, 5, 3, 2, 6, 1, 7)
MESH = pl.DeviceIdType.MESH
OUT_SPACE = pltpu.VMEM


def orders(ns):
    plans = []
    for eighths in (SLOW_EIGHTHS, FAST_EIGHTHS):
        plan = [e * ns // 8 + k for e in eighths for k in range(ns // 8)]
        plans.append(plan + [off for off in range(1, ns) if off not in plan])
    return plans


def deal_blocks(blocks, width):
    count = len(blocks)
    lane = lax.broadcasted_iota(jnp.int32, blocks[0].shape, 1) // width
    turned = [pltpu.roll(x, i * width, 1) if i else x for i, x in enumerate(blocks)]
    dealt = [turned[-k % count] for k in range(count)]
    step = 1
    while step < count:
        upper = (lane // step) % 2 == 1
        dealt = [jnp.where(upper, dealt[(k - step) % count], dealt[k]) for k in range(count)]
        step *= 2
    return dealt


def kernel(
    nf, ns, rows, spec,
    x_hbm, w_hbm, trig_hbm, god_hbm, own_hbm,
    out_ref,
    x_ref, w_ref, trig_ref, god_ref, own_ref,
    xf, send1, held, left, vis, tiles, mixed, send2, dev_of, table,
    lsem, row_sem, twin_sem, ssem1, rsem1, ssem2, rsem2,
):
    length = LANES
    ch_out = length // AVG
    spread = ns // ch_out
    rpf = ns // nf
    fl_count = ch_out // rpf
    chunks = spec // ch_out
    step = 2 * ch_out
    b = lax.axis_index("freq")
    me = lax.axis_index("stn")

    def load(n, src, dst):
        return pltpu.make_async_copy(src, dst, lsem.at[n])

    def load_x(th):
        return load(4 + th, x_hbm.at[:, th * step : (th + 1) * step, :], x_ref.at[th])

    load_w = load(0, w_hbm, w_ref)
    load_trig = load(1, trig_hbm, trig_ref)
    load_god = load(2, god_hbm, god_ref)
    load_own = load(3, own_hbm, own_ref)
    load_w.start()
    load_trig.start()
    for th in range(chunks):
        load_x(th).start()
    load_god.start()
    load_own.start()

    barrier = pltpu.get_barrier_semaphore()
    offsets = sorted(range(1, ns), key=lambda o: abs(o - ns / 2))
    for off in offsets:
        pl.semaphore_signal(
            barrier, inc=1, device_id=(b, lax.rem(me + off, ns)), device_id_type=MESH
        )
    for off in range(1, nf):
        pl.semaphore_signal(
            barrier, inc=1, device_id=(lax.rem(b + off, nf), me), device_id_type=MESH
        )

    load_w.wait()
    load_trig.wait()
    weights = jnp.broadcast_to(w_ref[...], (length, length)).T * (1.0 / math.sqrt(length))
    cosine = weights * trig_ref[0]
    sine = weights * trig_ref[1]
    matrix = jnp.concatenate(
        [jnp.concatenate([cosine, -sine], axis=1), jnp.concatenate([sine, cosine], axis=1)], axis=0
    )
    high = matrix.astype(jnp.bfloat16)
    low = (matrix - high.astype(jnp.float32)).astype(jnp.bfloat16)

    for th in range(chunks):
        load_x(th).wait()
    for th in range(chunks):
        xf[th] = x_ref[th].astype(jnp.float32).reshape(rows * step, length)
    for th in range(chunks):
        parts = []
        for t in range(ch_out):
            re = xf[th, pl.ds(2 * t, rows, stride=step), :]
            im = xf[th, pl.ds(2 * t + 1, rows, stride=step), :]
            parts.append(jnp.concatenate([re, im], axis=1).astype(jnp.bfloat16))
        flat = jnp.concatenate(parts, axis=0)
        spectra = jnp.dot(flat, high, preferred_element_type=jnp.float32) + jnp.dot(
            flat, low, preferred_element_type=jnp.float32
        )
        for p in range(2):
            blocks = [
                spectra[i * rows : (i + 1) * rows, p * LANES : (p + 1) * LANES]
                for i in range(ch_out)
            ]
            blocks = deal_blocks(blocks, AVG)
            for k in range(ch_out):
                send1[k, th, :, p * LANES : (p + 1) * LANES] = blocks[k].astype(jnp.bfloat16)

    def first_copy(d, mine):
        return pltpu.make_async_remote_copy(
            src_ref=send1.at[d // spread],
            dst_ref=held.at[mine],
            send_sem=ssem1.at[d],
            recv_sem=rsem1.at[mine],
            device_id=(b, d),
            device_id_type=MESH,
        )

    pl.semaphore_wait(barrier, ns - 1 + nf - 1)
    def start_first(offs):
        for off in offs:
            first_copy(lax.rem(me + off, ns), me).start()

    def end_first(offs):
        for off in offs:
            first_copy(lax.rem(me + off, ns), me).wait_send()

    slow = lax.rem(b, 2) == 0
    slow_order, fast_order = orders(ns)

    @pl.when(slow)
    def _():
        start_first(slow_order)
        end_first(slow_order[:LEAD])
        pl.semaphore_signal(twin_sem, inc=1, device_id=(b + 1, me), device_id_type=MESH)

    @pl.when(jnp.logical_not(slow))
    def _():
        start_first(fast_order[:HOLD])
        pl.semaphore_wait(twin_sem, 1)
        start_first(fast_order[HOLD:])

    for off in range(1, nf):
        pl.semaphore_signal(
            row_sem, inc=1, device_id=(lax.rem(b + off, nf), me), device_id_type=MESH
        )
    held[me] = send1[me // spread]

    load_god.wait()
    load_own.wait()

    def find_dev(g, carry):
        def body(s, acc):
            return jnp.where(god_ref[s] == g, s, acc)

        dev_of[g] = lax.fori_loop(0, ns, body, jnp.int32(0), unroll=min(ns, 8))
        return carry

    lax.fori_loop(0, ns, find_dev, 0)
    quarter = lax.rem(me, spread)

    def find_col(i, carry):
        g1 = quarter * ch_out + i // ns
        o = lax.rem(i, ns)

        def body(g2, acc):
            return jnp.where(own_ref[g1, g2] == o, dev_of[g2], acc)

        table[i] = lax.fori_loop(0, ns, body, jnp.int32(0), unroll=min(ns, 8))
        return carry

    lax.fori_loop(0, ch_out * ns, find_col, 0)
    pl.semaphore_wait(row_sem, nf - 1)

    channel = b * ch_out + me // spread
    first_row = quarter * fl_count

    def second_copy(fl, o):
        return pltpu.make_async_remote_copy(
            src_ref=send2.at[fl * ns + o],
            dst_ref=out_ref.at[:, channel],
            send_sem=ssem2.at[fl * ns + o],
            recv_sem=rsem2.at[channel],
            device_id=(first_row + fl, o),
            device_id_type=MESH,
        )

    def unless_mine(fl, o, run):
        mine = jnp.logical_and(first_row + fl == b, o == me)
        pl.when(jnp.logical_not(mine))(run)

    per_tile = LANES // rows
    sub = rows // per_tile
    span = rpf * rows
    wide = min(2 * per_tile, ns)
    cols = wide * rows

    def wait_first(i, carry):
        first_copy(me, lax.rem(me + i, ns)).wait_recv()
        return carry

    lax.fori_loop(1, ns, wait_first, 0)

    pair = 2 - fl_count % 2
    block_rows = 2 * span

    def correlate(f0):
        for u in range(pair):
            top = u * block_rows
            for g in range(rpf):
                x = held[dev_of[(first_row + f0 + u) * rpf + g]]
                at = top + g * rows
                for th in range(chunks):
                    left[th, at : at + rows, :] = x[th]
                    left[th, at + span : at + span + rows, :LANES] = x[th, :, LANES:]
                    left[th, at + span : at + span + rows, LANES:] = -x[th, :, :LANES]
        for c in range(ns // wide):
            for u in range(pair):
                block = sum(
                    lax.dot_general(
                        left[th, u * block_rows : (u + 1) * block_rows],
                        held[c * wide : (c + 1) * wide, th].reshape(cols, 2 * LANES),
                        (((1,), (1,)), ((), ())),
                        preferred_element_type=jnp.float32,
                    )
                    for th in range(chunks)
                ) * (1.0 / (AVG * spec))
                for h in range(cols // LANES):
                    vis[h, u * block_rows : (u + 1) * block_rows] = block[:, h * LANES : (h + 1) * LANES]
            for h in range(cols // LANES):
                blocks = [
                    vis[h, pl.ds(q, pair * block_rows // per_tile, stride=per_tile), :]
                    for q in range(per_tile)
                ]
                blocks = deal_blocks(blocks, rows)
                for s in range(per_tile):
                    whole = pltpu.roll(blocks[s], LANES - s * rows, 1) if s else blocks[s]
                    shaped = whole.reshape(pair, 2 * rpf, sub, LANES)
                    for u in range(pair):
                        tiles[f0 + u, c * wide + h * per_tile + s] = shaped[u]

    def build(fl, o):
        for g in range(rpf):
            source = table[(fl * rpf + g) * ns + o]
            for p in range(2):
                mixed[fl, o, p, pl.ds(g, sub, stride=rpf), :] = tiles[fl, source, p * rpf + g]
        for p in range(2):
            for r in range(sub):
                send2[fl * ns + o, p, :, r * LANES : (r + 1) * LANES] = mixed[
                    fl, o, p, r * rpf : (r + 1) * rpf, :
                ].astype(jnp.bfloat16)
        unless_mine(fl, o, lambda: second_copy(fl, o).start())

    for f0 in range(0, fl_count, pair):
        correlate(f0)

        def build_owner(o, carry):
            for u in range(pair):
                build(f0 + u, o)
            return carry

        lax.fori_loop(0, ns, build_owner, 0, unroll=min(ns, 8))

    own_here = quarter == b // fl_count

    @pl.when(own_here)
    def _():
        own = pltpu.make_async_copy(
            send2.at[lax.rem(b, fl_count) * ns + me], out_ref.at[:, channel], lsem.at[0]
        )
        own.start()
        own.wait()

    pl.when(slow)(lambda: end_first(slow_order[LEAD:]))
    pl.when(jnp.logical_not(slow))(lambda: end_first(fast_order))

    def arrived(slot):
        pltpu.make_async_remote_copy(
            src_ref=send2.at[0],
            dst_ref=out_ref.at[:, slot],
            send_sem=ssem2.at[0],
            recv_sem=rsem2.at[slot],
            device_id=(b, me),
            device_id_type=MESH,
        ).wait_recv()

    def wait_arrival(i, carry):
        arrived(lax.rem(channel + i, nf * ch_out))
        return carry

    pl.when(jnp.logical_not(own_here))(lambda: arrived(channel))
    lax.fori_loop(1, nf * ch_out, wait_arrival, 0)

    def wait_second(i, carry):
        fl, o = i // ns, lax.rem(i, ns)
        unless_mine(fl, o, lambda: second_copy(fl, o).wait_send())
        return carry

    lax.fori_loop(0, fl_count * ns, wait_second, 0)


def shards(nf, ns, samples, window, group_of_device, owner_map):
    _, rows, spec, _, length = samples.shape
    ch_out = length // AVG
    rpf = ns // nf
    fl_count = ch_out // rpf
    per_tile = LANES // rows
    sub = rows // per_tile
    chunks = spec // ch_out
    index = np.arange(length)
    theta = (index[:, None] * index[None, :] % length) * (2.0 * math.pi / length)
    trig = jnp.asarray(np.stack([np.cos(theta), np.sin(theta)]), jnp.float32)
    x = samples.reshape(rows, spec * 2, length)
    hbm = pl.BlockSpec(memory_space=pltpu.HBM)
    out = pl.pallas_call(
        functools.partial(kernel, nf, ns, rows, spec),
        out_shape=pltpu.VMEM((2, nf * ch_out, rpf, sub * LANES), jnp.bfloat16),
        in_specs=[hbm] * 5,
        out_specs=pl.BlockSpec(memory_space=OUT_SPACE),
        scratch_shapes=[
            pltpu.VMEM((chunks, rows, 2 * ch_out, length), jnp.bfloat16),
            pltpu.VMEM((1, length), jnp.float32),
            pltpu.VMEM((2, length, length), jnp.float32),
            pltpu.SMEM((ns,), jnp.int32),
            pltpu.SMEM((ns, ns), jnp.int32),
            pltpu.VMEM((chunks, rows * 2 * ch_out, length), jnp.float32),
            pltpu.VMEM((ch_out, chunks, rows, 2 * LANES), jnp.bfloat16),
            pltpu.VMEM((ns, chunks, rows, 2 * LANES), jnp.bfloat16),
            pltpu.VMEM((chunks, 4 * rpf * rows, 2 * LANES), jnp.bfloat16),
            pltpu.VMEM((2, 4 * rpf * rows, LANES), jnp.float32),
            pltpu.VMEM((fl_count, ns, 2 * rpf, sub, LANES), jnp.float32),
            pltpu.VMEM((fl_count, ns, 2, sub * rpf, LANES), jnp.float32),
            pltpu.VMEM((fl_count * ns, 2, rpf, sub * LANES), jnp.bfloat16),
            pltpu.SMEM((ns,), jnp.int32),
            pltpu.SMEM((ch_out * ns,), jnp.int32),
            pltpu.SemaphoreType.DMA((4 + chunks,)),
            pltpu.SemaphoreType.REGULAR,
            pltpu.SemaphoreType.REGULAR,
            pltpu.SemaphoreType.DMA((ns,)),
            pltpu.SemaphoreType.DMA((ns,)),
            pltpu.SemaphoreType.DMA((fl_count * ns,)),
            pltpu.SemaphoreType.DMA((nf * ch_out,)),
        ],
        compiler_params=pltpu.CompilerParams(
            collective_id=0, has_side_effects=True, vmem_limit_bytes=60 * 1024 * 1024
        ),
    )(x, window.reshape(1, length), trig, group_of_device, owner_map)
    return out[:, :, None]


def solution(mesh):
    return jax.shard_map(
        functools.partial(shards, mesh.shape["freq"], mesh.shape["stn"]),
        mesh=mesh,
        in_specs=(P("freq", "stn", None, None, None), P(), P(), P()),
        out_specs=P(None, None, "stn", "freq", None),
        check_vma=False,
    )
```

```python
import functools
import math

import jax
import jax.numpy as jnp
import numpy as np
from jax import lax
from jax.experimental import pallas as pl
from jax.experimental.pallas import tpu as pltpu
from jax.sharding import PartitionSpec as P

AVG = 16
LANES = 128
LEAD = 3
HOLD = 1
SLOW_EIGHTHS = (4, 3, 5, 2, 1, 6, 7)
FAST_EIGHTHS = (4, 5, 3, 2, 6, 1, 7)
MESH = pl.DeviceIdType.MESH
OUT_SPACE = pltpu.VMEM


def orders(ns):
    plans = []
    for eighths in (SLOW_EIGHTHS, FAST_EIGHTHS):
        plan = [e * ns // 8 + k for e in eighths for k in range(ns // 8)]
        plans.append(plan + [off for off in range(1, ns) if off not in plan])
    return plans


def deal_blocks(blocks, width):
    count = len(blocks)
    lane = lax.broadcasted_iota(jnp.int32, blocks[0].shape, 1) // width
    turned = [pltpu.roll(x, i * width, 1) if i else x for i, x in enumerate(blocks)]
    dealt = [turned[-k % count] for k in range(count)]
    step = 1
    while step < count:
        upper = (lane // step) % 2 == 1
        dealt = [jnp.where(upper, dealt[(k - step) % count], dealt[k]) for k in range(count)]
        step *= 2
    return dealt


def kernel(
    nf, ns, rows, spec,
    x_hbm, w_hbm, trig_hbm, god_hbm, own_hbm,
    out_ref,
    x_ref, w_ref, trig_ref, god_ref, own_ref,
    xf, send1, held, left, vis, tiles, mixed, send2, dev_of, table,
    lsem, row_sem, twin_sem, ssem1, rsem1, ssem2, rsem2,
):
    length = LANES
    ch_out = length // AVG
    spread = ns // ch_out
    rpf = ns // nf
    fl_count = ch_out // rpf
    chunks = spec // ch_out
    step = 2 * ch_out
    b = lax.axis_index("freq")
    me = lax.axis_index("stn")

    def load(n, src, dst):
        return pltpu.make_async_copy(src, dst, lsem.at[n])

    def load_x(th):
        return load(4 + th, x_hbm.at[:, th * step : (th + 1) * step, :], x_ref.at[th])

    load_w = load(0, w_hbm, w_ref)
    load_trig = load(1, trig_hbm, trig_ref)
    load_god = load(2, god_hbm, god_ref)
    load_own = load(3, own_hbm, own_ref)
    load_w.start()
    load_trig.start()
    for th in range(chunks):
        load_x(th).start()
    load_god.start()
    load_own.start()

    barrier = pltpu.get_barrier_semaphore()
    offsets = sorted(range(1, ns), key=lambda o: abs(o - ns / 2))
    for off in offsets:
        pl.semaphore_signal(
            barrier, inc=1, device_id=(b, lax.rem(me + off, ns)), device_id_type=MESH
        )
    for off in range(1, nf):
        pl.semaphore_signal(
            barrier, inc=1, device_id=(lax.rem(b + off, nf), me), device_id_type=MESH
        )

    load_w.wait()
    load_trig.wait()
    weights = jnp.broadcast_to(w_ref[...], (length, length)).T * (1.0 / math.sqrt(length))
    cosine = weights * trig_ref[0]
    sine = weights * trig_ref[1]
    matrix = jnp.concatenate(
        [jnp.concatenate([cosine, -sine], axis=1), jnp.concatenate([sine, cosine], axis=1)], axis=0
    )
    high = matrix.astype(jnp.bfloat16)
    low = (matrix - high.astype(jnp.float32)).astype(jnp.bfloat16)

    for th in range(chunks):
        load_x(th).wait()
    for th in range(chunks):
        xf[th] = x_ref[th].astype(jnp.float32).reshape(rows * step, length)
    for th in range(chunks):
        parts = []
        for t in range(ch_out):
            re = xf[th, pl.ds(2 * t, rows, stride=step), :]
            im = xf[th, pl.ds(2 * t + 1, rows, stride=step), :]
            parts.append(jnp.concatenate([re, im], axis=1).astype(jnp.bfloat16))
        flat = jnp.concatenate(parts, axis=0)
        spectra = jnp.dot(flat, high, preferred_element_type=jnp.float32) + jnp.dot(
            flat, low, preferred_element_type=jnp.float32
        )
        for p in range(2):
            blocks = [
                spectra[i * rows : (i + 1) * rows, p * LANES : (p + 1) * LANES]
                for i in range(ch_out)
            ]
            blocks = deal_blocks(blocks, AVG)
            for k in range(ch_out):
                send1[k, th, :, p * LANES : (p + 1) * LANES] = blocks[k].astype(jnp.bfloat16)

    def whole(ref, sem):
        return pltpu.make_async_copy(ref, ref, sem.at[0])

    def first_copy(d, mine):
        return pltpu.make_async_remote_copy(
            src_ref=send1.at[d // spread],
            dst_ref=held.at[mine],
            send_sem=ssem1.at[d],
            recv_sem=rsem1.at[0],
            device_id=(b, d),
            device_id_type=MESH,
        )

    pl.semaphore_wait(barrier, ns - 1 + nf - 1)
    def start_first(offs):
        for off in offs:
            first_copy(lax.rem(me + off, ns), me).start()

    def end_first(offs):
        for off in offs:
            first_copy(lax.rem(me + off, ns), me).wait_send()

    slow = lax.rem(b, 2) == 0
    slow_order, fast_order = orders(ns)

    @pl.when(slow)
    def _():
        start_first(slow_order)
        end_first(slow_order[:LEAD])
        pl.semaphore_signal(twin_sem, inc=1, device_id=(b + 1, me), device_id_type=MESH)

    @pl.when(jnp.logical_not(slow))
    def _():
        start_first(fast_order[:HOLD])
        pl.semaphore_wait(twin_sem, 1)
        start_first(fast_order[HOLD:])

    for off in range(1, nf):
        pl.semaphore_signal(
            row_sem, inc=1, device_id=(lax.rem(b + off, nf), me), device_id_type=MESH
        )
    held[me] = send1[me // spread]

    load_god.wait()
    load_own.wait()

    def find_dev(g, carry):
        def body(s, acc):
            return jnp.where(god_ref[s] == g, s, acc)

        dev_of[g] = lax.fori_loop(0, ns, body, jnp.int32(0), unroll=min(ns, 8))
        return carry

    lax.fori_loop(0, ns, find_dev, 0)
    quarter = lax.rem(me, spread)

    def find_col(i, carry):
        g1 = quarter * ch_out + i // ns
        o = lax.rem(i, ns)

        def body(g2, acc):
            return jnp.where(own_ref[g1, g2] == o, dev_of[g2], acc)

        table[i] = lax.fori_loop(0, ns, body, jnp.int32(0), unroll=min(ns, 8))
        return carry

    lax.fori_loop(0, ch_out * ns, find_col, 0)
    pl.semaphore_wait(row_sem, nf - 1)

    channel = b * ch_out + me // spread
    first_row = quarter * fl_count

    def second_copy(fl, o):
        return pltpu.make_async_remote_copy(
            src_ref=send2.at[fl * ns + o],
            dst_ref=out_ref.at[:, channel],
            send_sem=ssem2.at[0],
            recv_sem=rsem2.at[0],
            device_id=(first_row + fl, o),
            device_id_type=MESH,
        )

    def unless_mine(fl, o, run):
        mine = jnp.logical_and(first_row + fl == b, o == me)
        pl.when(jnp.logical_not(mine))(run)

    per_tile = LANES // rows
    sub = rows // per_tile
    span = rpf * rows
    wide = min(2 * per_tile, ns)
    cols = wide * rows

    whole(held.at[: ns - 1], rsem1).wait()

    pair = 2 - fl_count % 2
    block_rows = 2 * span

    def correlate(f0):
        for u in range(pair):
            top = u * block_rows
            for g in range(rpf):
                x = held[dev_of[(first_row + f0 + u) * rpf + g]]
                at = top + g * rows
                for th in range(chunks):
                    left[th, at : at + rows, :] = x[th]
                    left[th, at + span : at + span + rows, :LANES] = x[th, :, LANES:]
                    left[th, at + span : at + span + rows, LANES:] = -x[th, :, :LANES]
        for c in range(ns // wide):
            for u in range(pair):
                block = sum(
                    lax.dot_general(
                        left[th, u * block_rows : (u + 1) * block_rows],
                        held[c * wide : (c + 1) * wide, th].reshape(cols, 2 * LANES),
                        (((1,), (1,)), ((), ())),
                        preferred_element_type=jnp.float32,
                    )
                    for th in range(chunks)
                ) * (1.0 / (AVG * spec))
                for h in range(cols // LANES):
                    vis[h, u * block_rows : (u + 1) * block_rows] = block[:, h * LANES : (h + 1) * LANES]
            for h in range(cols // LANES):
                blocks = [
                    vis[h, pl.ds(q, pair * block_rows // per_tile, stride=per_tile), :]
                    for q in range(per_tile)
                ]
                blocks = deal_blocks(blocks, rows)
                for s in range(per_tile):
                    whole = pltpu.roll(blocks[s], LANES - s * rows, 1) if s else blocks[s]
                    shaped = whole.reshape(pair, 2 * rpf, sub, LANES)
                    for u in range(pair):
                        tiles[f0 + u, c * wide + h * per_tile + s] = shaped[u]

    def build(fl, o):
        for g in range(rpf):
            source = table[(fl * rpf + g) * ns + o]
            for p in range(2):
                mixed[fl, o, p, pl.ds(g, sub, stride=rpf), :] = tiles[fl, source, p * rpf + g]
        for p in range(2):
            for r in range(sub):
                send2[fl * ns + o, p, :, r * LANES : (r + 1) * LANES] = mixed[
                    fl, o, p, r * rpf : (r + 1) * rpf, :
                ].astype(jnp.bfloat16)
        unless_mine(fl, o, lambda: second_copy(fl, o).start())

    for f0 in range(0, fl_count, pair):
        correlate(f0)

        def build_owner(o, carry):
            for u in range(pair):
                build(f0 + u, o)
            return carry

        lax.fori_loop(0, ns, build_owner, 0, unroll=min(ns, 8))

    own_here = quarter == b // fl_count

    @pl.when(own_here)
    def _():
        own = pltpu.make_async_copy(
            send2.at[lax.rem(b, fl_count) * ns + me], out_ref.at[:, channel], lsem.at[0]
        )
        own.start()
        own.wait()

    pl.when(slow)(lambda: end_first(slow_order[LEAD:]))
    pl.when(jnp.logical_not(slow))(lambda: end_first(fast_order))

    def end_second(count):
        whole(send2.at[:count], ssem2).wait()
        whole(out_ref.at[:, :count], rsem2).wait()

    pl.when(own_here)(lambda: end_second(nf * ch_out - 1))
    pl.when(jnp.logical_not(own_here))(lambda: end_second(nf * ch_out))


def shards(nf, ns, samples, window, group_of_device, owner_map):
    _, rows, spec, _, length = samples.shape
    ch_out = length // AVG
    rpf = ns // nf
    fl_count = ch_out // rpf
    per_tile = LANES // rows
    sub = rows // per_tile
    chunks = spec // ch_out
    index = np.arange(length)
    theta = (index[:, None] * index[None, :] % length) * (2.0 * math.pi / length)
    trig = jnp.asarray(np.stack([np.cos(theta), np.sin(theta)]), jnp.float32)
    x = samples.reshape(rows, spec * 2, length)
    hbm = pl.BlockSpec(memory_space=pltpu.HBM)
    out = pl.pallas_call(
        functools.partial(kernel, nf, ns, rows, spec),
        out_shape=pltpu.VMEM((2, nf * ch_out, rpf, sub * LANES), jnp.bfloat16),
        in_specs=[hbm] * 5,
        out_specs=pl.BlockSpec(memory_space=OUT_SPACE),
        scratch_shapes=[
            pltpu.VMEM((chunks, rows, 2 * ch_out, length), jnp.bfloat16),
            pltpu.VMEM((1, length), jnp.float32),
            pltpu.VMEM((2, length, length), jnp.float32),
            pltpu.SMEM((ns,), jnp.int32),
            pltpu.SMEM((ns, ns), jnp.int32),
            pltpu.VMEM((chunks, rows * 2 * ch_out, length), jnp.float32),
            pltpu.VMEM((ch_out, chunks, rows, 2 * LANES), jnp.bfloat16),
            pltpu.VMEM((ns, chunks, rows, 2 * LANES), jnp.bfloat16),
            pltpu.VMEM((chunks, 4 * rpf * rows, 2 * LANES), jnp.bfloat16),
            pltpu.VMEM((2, 4 * rpf * rows, LANES), jnp.float32),
            pltpu.VMEM((fl_count, ns, 2 * rpf, sub, LANES), jnp.float32),
            pltpu.VMEM((fl_count, ns, 2, sub * rpf, LANES), jnp.float32),
            pltpu.VMEM((fl_count * ns, 2, rpf, sub * LANES), jnp.bfloat16),
            pltpu.SMEM((ns,), jnp.int32),
            pltpu.SMEM((ch_out * ns,), jnp.int32),
            pltpu.SemaphoreType.DMA((4 + chunks,)),
            pltpu.SemaphoreType.REGULAR,
            pltpu.SemaphoreType.REGULAR,
            pltpu.SemaphoreType.DMA((ns,)),
            pltpu.SemaphoreType.DMA((1,)),
            pltpu.SemaphoreType.DMA((1,)),
            pltpu.SemaphoreType.DMA((1,)),
        ],
        compiler_params=pltpu.CompilerParams(
            collective_id=0, has_side_effects=True, vmem_limit_bytes=60 * 1024 * 1024
        ),
    )(x, window.reshape(1, length), trig, group_of_device, owner_map)
    return out[:, :, None]


def solution(mesh):
    return jax.shard_map(
        functools.partial(shards, mesh.shape["freq"], mesh.shape["stn"]),
        mesh=mesh,
        in_specs=(P("freq", "stn", None, None, None), P(), P(), P()),
        out_specs=P(None, None, "stn", "freq", None),
        check_vma=False,
    )
```

```python
import functools
import math

import jax
import jax.numpy as jnp
import numpy as np
from jax import lax
from jax.experimental import pallas as pl
from jax.experimental.pallas import tpu as pltpu
from jax.sharding import PartitionSpec as P

AVG = 16
LANES = 128
PLANES = 4
PLANS = (
    (
        ((1, 0), 'h2', (2, 0), 'h3', (3, 0), (3, 1), (1, 1), (2, 1), (0, 1), (0, 0), ('tell', 3)),
        ((1, 0), 'h2', 'h3', 'wait', (1, 1), (2, 0), (3, 0), (3, 1), (2, 1), (0, 0), (0, 1)),
    ),
    (
        ((2, 1), 'h2', (3, 0), (3, 1), (2, 0), (0, 0), (1, 1), (0, 1), (1, 0), ('tell', 3)),
        ((2, 1), 'h2', 'wait', (3, 1), (3, 0), (2, 0), (0, 0), (0, 1), (1, 1), (1, 0)),
    ),
    (
        ((2, 1), 'h2', (3, 1), (3, 0), (2, 0), (0, 0), (0, 1), (1, 1), (1, 0)),
        ((2, 1), 'h2', (3, 1), (3, 0), (2, 0), (0, 0), (1, 1), (0, 1), (1, 0)),
    ),
    (
        ((1, 0), 'h2', (2, 0), 'h3', (3, 0), (3, 1), (1, 1), (2, 1), (0, 1), (0, 0)),
        ((1, 0), 'h2', (2, 0), 'h3', (3, 0), (3, 1), (1, 1), (2, 1), (0, 1), (0, 0)),
    ),
)
MESH = pl.DeviceIdType.MESH
OUT_SPACE = pltpu.VMEM


def deal_blocks(blocks, width):
    count = len(blocks)
    lane = lax.broadcasted_iota(jnp.int32, blocks[0].shape, 1) // width
    turned = [pltpu.roll(x, i * width, 1) if i else x for i, x in enumerate(blocks)]
    dealt = [turned[-k % count] for k in range(count)]
    step = 1
    while step < count:
        upper = (lane // step) % 2 == 1
        dealt = [jnp.where(upper, dealt[(k - step) % count], dealt[k]) for k in range(count)]
        step *= 2
    return dealt


def kernel(
    nf, ns, rows, spec,
    x_hbm, w_hbm, trig_hbm, god_hbm, own_hbm,
    out_ref,
    x_ref, w_ref, trig_ref, god_ref, own_ref,
    xf, send1, held, left, vis, tiles, mixed, send2, dev_of, table,
    lsem, row_sem, hop_sem, twin_sem, ssem1, rsem1, ssem2, rsem2,
):
    length = LANES
    ch_out = length // AVG
    spread = ns // ch_out
    rpf = ns // nf
    fl_count = ch_out // rpf
    chunks = spec // ch_out
    step = 2 * ch_out
    lanes = ns // PLANES
    b = lax.axis_index("freq")
    me = lax.axis_index("stn")
    plane = me // lanes
    lane = lax.rem(me, lanes)

    def load(n, src, dst):
        return pltpu.make_async_copy(src, dst, lsem.at[n])

    def load_x(th):
        return load(4, x_hbm.at[:, th * step : (th + 1) * step, :], x_ref.at[th])

    load_w = load(0, w_hbm, w_ref)
    load_trig = load(1, trig_hbm, trig_ref)
    load_god = load(2, god_hbm, god_ref)
    load_own = load(3, own_hbm, own_ref)

    barrier = pltpu.get_barrier_semaphore()
    def mate(delta, r):
        return (plane + delta) * lanes + lax.rem(lane + r, lanes)

    def greet(delta):
        for r in range(lanes):
            if delta or r:
                pl.semaphore_signal(
                    barrier, inc=1, device_id=(b, mate(delta, r)), device_id_type=MESH
                )

    for delta in (1, -1):
        far = plane + delta
        pl.when(jnp.logical_and(far >= 0, far < PLANES))(functools.partial(greet, delta))
    greet(0)
    for off in range(1, nf):
        pl.semaphore_signal(
            barrier, inc=1, device_id=(lax.rem(b + off, nf), me), device_id_type=MESH
        )

    load_w.start()
    load_trig.start()
    for th in range(chunks):
        load_x(th).start()
    load_god.start()
    load_own.start()

    load_w.wait()
    load_trig.wait()
    weights = jnp.broadcast_to(w_ref[...], (length, length)).T * (1.0 / math.sqrt(length))
    cosine = weights * trig_ref[0]
    sine = weights * trig_ref[1]
    matrix = jnp.concatenate(
        [jnp.concatenate([cosine, -sine], axis=1), jnp.concatenate([sine, cosine], axis=1)], axis=0
    )
    high = matrix.astype(jnp.bfloat16)
    low = (matrix - high.astype(jnp.float32)).astype(jnp.bfloat16)

    load(4, x_ref, x_ref).wait()
    for th in range(chunks):
        xf[th] = x_ref[th].astype(jnp.float32).reshape(rows * step, length)
    for th in range(chunks):
        parts = []
        for t in range(ch_out):
            re = xf[th, pl.ds(2 * t, rows, stride=step), :]
            im = xf[th, pl.ds(2 * t + 1, rows, stride=step), :]
            parts.append(jnp.concatenate([re, im], axis=1).astype(jnp.bfloat16))
        flat = jnp.concatenate(parts, axis=0)
        spectra = jnp.dot(flat, high, preferred_element_type=jnp.float32) + jnp.dot(
            flat, low, preferred_element_type=jnp.float32
        )
        for p in range(2):
            blocks = [
                spectra[i * rows : (i + 1) * rows, p * LANES : (p + 1) * LANES]
                for i in range(ch_out)
            ]
            blocks = deal_blocks(blocks, AVG)
            for k in range(ch_out):
                send1[k, th, :, p * LANES : (p + 1) * LANES] = blocks[k].astype(jnp.bfloat16)

    def whole(ref, sem):
        return pltpu.make_async_copy(ref, ref, sem.at[0])

    def first_copy(d, mine):
        return pltpu.make_async_remote_copy(
            src_ref=send1.at[d // spread],
            dst_ref=held.at[mine],
            send_sem=ssem1.at[d],
            recv_sem=rsem1.at[0],
            device_id=(b, d),
            device_id_type=MESH,
        )

    def tell(distance, delta):
        pl.semaphore_signal(
            hop_sem.at[2 * (distance - 2) + (delta < 0)], inc=1,
            device_id=(b, mate(-delta, 0)), device_id_type=MESH,
        )

    def hear(distance, delta):
        pl.semaphore_wait(hop_sem.at[2 * (distance - 2) + (delta < 0)], 1)

    def targets(at, entry):
        to = entry[0] if 2 * at < PLANES else PLANES - 1 - entry[0]
        return [mate(to - at, r) for r in range(entry[1], lanes, 2) if to != at or r]

    def is_send(entry):
        return isinstance(entry, tuple) and entry[0] != "tell"

    def each_role(run):
        for at in range(PLANES):
            inner = 0 < at < PLANES - 1
            for half in range(2):
                pl.when(jnp.logical_and(plane == at, lax.rem(b, 2) == half))(
                    functools.partial(run, at, inner, PLANS[at][half])
                )

    def send_first(at, inner, plan):
        up = 1 if 2 * at < PLANES else -1
        pl.semaphore_wait(barrier, (3 if inner else 2) * lanes - 1 + nf - 1)
        if inner:
            tell(2, up)
            tell(2, -up)
        for entry in plan:
            if entry == "h2":
                hear(2, up)
                if inner:
                    tell(3, up)
            elif entry == "h3":
                hear(3, up)
            elif entry == "wait":
                pl.semaphore_wait(twin_sem, 1)
            elif is_send(entry):
                for d in targets(at, entry):
                    first_copy(d, me).start()
            else:
                for sent in list(filter(is_send, plan))[: entry[1]]:
                    for d in targets(at, sent):
                        first_copy(d, me).wait_send()
                pl.semaphore_signal(
                    twin_sem, inc=1, device_id=(b + 1 - 2 * lax.rem(b, 2), me), device_id_type=MESH
                )

    each_role(send_first)

    for off in range(1, nf):
        pl.semaphore_signal(
            row_sem, inc=1, device_id=(lax.rem(b + off, nf), me), device_id_type=MESH
        )
    held[me] = send1[me // spread]

    load_god.wait()
    load_own.wait()

    def find_dev(g, carry):
        def body(s, acc):
            return jnp.where(god_ref[s] == g, s, acc)

        dev_of[g] = lax.fori_loop(0, ns, body, jnp.int32(0), unroll=min(ns, 8))
        return carry

    lax.fori_loop(0, ns, find_dev, 0)
    quarter = lax.rem(me, spread)

    def find_col(i, carry):
        g1 = quarter * ch_out + i // ns
        o = lax.rem(i, ns)

        def body(g2, acc):
            return jnp.where(own_ref[g1, g2] == o, dev_of[g2], acc)

        table[i] = lax.fori_loop(0, ns, body, jnp.int32(0), unroll=min(ns, 8))
        return carry

    lax.fori_loop(0, ch_out * ns, find_col, 0)
    pl.semaphore_wait(row_sem, nf - 1)

    channel = b * ch_out + me // spread
    first_row = quarter * fl_count

    def second_copy(fl, o):
        return pltpu.make_async_remote_copy(
            src_ref=send2.at[fl * ns + o],
            dst_ref=out_ref.at[:, channel],
            send_sem=ssem2.at[0],
            recv_sem=rsem2.at[0],
            device_id=(first_row + fl, o),
            device_id_type=MESH,
        )

    def unless_mine(fl, o, run):
        mine = jnp.logical_and(first_row + fl == b, o == me)
        pl.when(jnp.logical_not(mine))(run)

    per_tile = LANES // rows
    sub = rows // per_tile
    span = rpf * rows
    wide = min(2 * per_tile, ns)
    cols = wide * rows

    whole(held.at[: ns - 1], rsem1).wait()

    pair = 2 - fl_count % 2
    block_rows = 2 * span

    def correlate(f0):
        for u in range(pair):
            top = u * block_rows
            for g in range(rpf):
                x = held[dev_of[(first_row + f0 + u) * rpf + g]]
                at = top + g * rows
                for th in range(chunks):
                    left[th, at : at + rows, :] = x[th]
                    left[th, at + span : at + span + rows, :LANES] = x[th, :, LANES:]
                    left[th, at + span : at + span + rows, LANES:] = -x[th, :, :LANES]
        for c in range(ns // wide):
            for u in range(pair):
                block = sum(
                    lax.dot_general(
                        left[th, u * block_rows : (u + 1) * block_rows],
                        held[c * wide : (c + 1) * wide, th].reshape(cols, 2 * LANES),
                        (((1,), (1,)), ((), ())),
                        preferred_element_type=jnp.float32,
                    )
                    for th in range(chunks)
                ) * (1.0 / (AVG * spec))
                for h in range(cols // LANES):
                    vis[h, u * block_rows : (u + 1) * block_rows] = block[:, h * LANES : (h + 1) * LANES]
            for h in range(cols // LANES):
                blocks = [
                    vis[h, pl.ds(q, pair * block_rows // per_tile, stride=per_tile), :]
                    for q in range(per_tile)
                ]
                blocks = deal_blocks(blocks, rows)
                for s in range(per_tile):
                    whole = pltpu.roll(blocks[s], LANES - s * rows, 1) if s else blocks[s]
                    shaped = whole.reshape(pair, 2 * rpf, sub, LANES)
                    for u in range(pair):
                        tiles[f0 + u, c * wide + h * per_tile + s] = shaped[u]

    def build(fl, o):
        for g in range(rpf):
            source = table[(fl * rpf + g) * ns + o]
            for p in range(2):
                mixed[fl, o, p, pl.ds(g, sub, stride=rpf), :] = tiles[fl, source, p * rpf + g]
        for p in range(2):
            for r in range(sub):
                send2[fl * ns + o, p, :, r * LANES : (r + 1) * LANES] = mixed[
                    fl, o, p, r * rpf : (r + 1) * rpf, :
                ].astype(jnp.bfloat16)
        unless_mine(fl, o, lambda: second_copy(fl, o).start())

    for f0 in range(0, fl_count, pair):
        correlate(f0)

        def build_owner(o, carry):
            for u in range(pair):
                build(f0 + u, o)
            return carry

        lax.fori_loop(0, ns, build_owner, 0, unroll=min(ns, 8))

    own_here = quarter == b // fl_count

    @pl.when(own_here)
    def _():
        own = pltpu.make_async_copy(
            send2.at[lax.rem(b, fl_count) * ns + me], out_ref.at[:, channel], lsem.at[0]
        )
        own.start()
        own.wait()

    def end_first(at, inner, plan):
        done = sum(entry[1] for entry in plan if not is_send(entry) and entry[0] == "tell")
        for entry in list(filter(is_send, plan))[done:]:
            for d in targets(at, entry):
                first_copy(d, me).wait_send()

    each_role(end_first)

    def end_second(count):
        whole(send2.at[:count], ssem2).wait()
        whole(out_ref.at[:, :count], rsem2).wait()

    pl.when(own_here)(lambda: end_second(nf * ch_out - 1))
    pl.when(jnp.logical_not(own_here))(lambda: end_second(nf * ch_out))


def shards(nf, ns, samples, window, group_of_device, owner_map):
    _, rows, spec, _, length = samples.shape
    ch_out = length // AVG
    rpf = ns // nf
    fl_count = ch_out // rpf
    per_tile = LANES // rows
    sub = rows // per_tile
    chunks = spec // ch_out
    index = np.arange(length)
    theta = (index[:, None] * index[None, :] % length) * (2.0 * math.pi / length)
    trig = jnp.asarray(np.stack([np.cos(theta), np.sin(theta)]), jnp.float32)
    x = samples.reshape(rows, spec * 2, length)
    hbm = pl.BlockSpec(memory_space=pltpu.HBM)
    out = pl.pallas_call(
        functools.partial(kernel, nf, ns, rows, spec),
        out_shape=pltpu.VMEM((2, nf * ch_out, rpf, sub * LANES), jnp.bfloat16),
        in_specs=[hbm] * 5,
        out_specs=pl.BlockSpec(memory_space=OUT_SPACE),
        scratch_shapes=[
            pltpu.VMEM((chunks, rows, 2 * ch_out, length), jnp.bfloat16),
            pltpu.VMEM((1, length), jnp.float32),
            pltpu.VMEM((2, length, length), jnp.float32),
            pltpu.SMEM((ns,), jnp.int32),
            pltpu.SMEM((ns, ns), jnp.int32),
            pltpu.VMEM((chunks, rows * 2 * ch_out, length), jnp.float32),
            pltpu.VMEM((ch_out, chunks, rows, 2 * LANES), jnp.bfloat16),
            pltpu.VMEM((ns, chunks, rows, 2 * LANES), jnp.bfloat16),
            pltpu.VMEM((chunks, 4 * rpf * rows, 2 * LANES), jnp.bfloat16),
            pltpu.VMEM((2, 4 * rpf * rows, LANES), jnp.float32),
            pltpu.VMEM((fl_count, ns, 2 * rpf, sub, LANES), jnp.float32),
            pltpu.VMEM((fl_count, ns, 2, sub * rpf, LANES), jnp.float32),
            pltpu.VMEM((fl_count * ns, 2, rpf, sub * LANES), jnp.bfloat16),
            pltpu.SMEM((ns,), jnp.int32),
            pltpu.SMEM((ch_out * ns,), jnp.int32),
            pltpu.SemaphoreType.DMA((5,)),
            pltpu.SemaphoreType.REGULAR,
            pltpu.SemaphoreType.REGULAR((2 * (PLANES - 2),)),
            pltpu.SemaphoreType.REGULAR,
            pltpu.SemaphoreType.DMA((ns,)),
            pltpu.SemaphoreType.DMA((1,)),
            pltpu.SemaphoreType.DMA((1,)),
            pltpu.SemaphoreType.DMA((1,)),
        ],
        compiler_params=pltpu.CompilerParams(
            collective_id=0, has_side_effects=True, vmem_limit_bytes=60 * 1024 * 1024
        ),
    )(x, window.reshape(1, length), trig, group_of_device, owner_map)
    return out[:, :, None]


def solution(mesh):
    return jax.shard_map(
        functools.partial(shards, mesh.shape["freq"], mesh.shape["stn"]),
        mesh=mesh,
        in_specs=(P("freq", "stn", None, None, None), P(), P(), P()),
        out_specs=P(None, None, "stn", "freq", None),
        check_vma=False,
    )
```

```python
import functools
import math

import jax
import jax.numpy as jnp
import numpy as np
from jax import lax
from jax.experimental import pallas as pl
from jax.experimental.pallas import tpu as pltpu
from jax.sharding import PartitionSpec as P

AVG = 16
LANES = 128
PLANES = 4
PLANS = (
    (
        ((1, 0), 'h2', (2, 0), 'h3', (3, 0), (3, 1), (1, 1), (2, 1), (0, 1), (0, 0), ('tell', 3)),
        ((1, 0), 'h2', 'h3', 'wait', (1, 1), (2, 0), (3, 0), (3, 1), (2, 1), (0, 0), (0, 1)),
    ),
    (
        ((2, 1), 'h2', (3, 0), (3, 1), (2, 0), (0, 0), (1, 1), (0, 1), (1, 0), ('tell', 3)),
        ((2, 1), 'h2', 'wait', (3, 1), (3, 0), (2, 0), (0, 0), (0, 1), (1, 1), (1, 0)),
    ),
    (
        ((2, 1), 'h2', (3, 1), (3, 0), (2, 0), (0, 0), (0, 1), (1, 1), (1, 0)),
        ((2, 1), 'h2', (3, 1), (3, 0), (2, 0), (0, 0), (1, 1), (0, 1), (1, 0)),
    ),
    (
        ((1, 0), 'h2', (2, 0), 'h3', (3, 0), (3, 1), (1, 1), (2, 1), (0, 1), (0, 0)),
        ((1, 0), 'h2', (2, 0), 'h3', (3, 0), (3, 1), (1, 1), (2, 1), (0, 1), (0, 0)),
    ),
)
MESH = pl.DeviceIdType.MESH
OUT_SPACE = pltpu.VMEM


def deal_blocks(blocks, width):
    count = len(blocks)
    lane = lax.broadcasted_iota(jnp.int32, blocks[0].shape, 1) // width
    turned = [pltpu.roll(x, i * width, 1) if i else x for i, x in enumerate(blocks)]
    dealt = [turned[-k % count] for k in range(count)]
    step = 1
    while step < count:
        upper = (lane // step) % 2 == 1
        dealt = [jnp.where(upper, dealt[(k - step) % count], dealt[k]) for k in range(count)]
        step *= 2
    return dealt


def kernel(
    nf, ns, rows, spec,
    x_hbm, w_hbm, trig_hbm, god_hbm, own_hbm,
    out_ref,
    x_ref, w_ref, trig_ref, god_ref, own_ref,
    xf, send1, held, left, vis, tiles, mixed, send2, dev_of, table,
    lsem, row_sem, hop_sem, twin_sem, ssem1, rsem1, ssem2, rsem2,
):
    length = LANES
    ch_out = length // AVG
    spread = ns // ch_out
    rpf = ns // nf
    fl_count = ch_out // rpf
    chunks = spec // ch_out
    step = 2 * ch_out
    lanes = ns // PLANES
    b = lax.axis_index("freq")
    me = lax.axis_index("stn")
    plane = me // lanes
    lane = lax.rem(me, lanes)

    def load(n, src, dst):
        return pltpu.make_async_copy(src, dst, lsem.at[n])

    def load_x(th):
        return load(4, x_hbm.at[:, th * step : (th + 1) * step, :], x_ref.at[th])

    load_w = load(0, w_hbm, w_ref)
    load_trig = load(1, trig_hbm, trig_ref)
    load_god = load(2, god_hbm, god_ref)
    load_own = load(3, own_hbm, own_ref)

    barrier = pltpu.get_barrier_semaphore()
    def mate(delta, r):
        return (plane + delta) * lanes + lax.rem(lane + r, lanes)

    def greet(delta):
        for r in range(lanes):
            if delta or r:
                pl.semaphore_signal(
                    barrier, inc=1, device_id=(b, mate(delta, r)), device_id_type=MESH
                )

    for delta in (1, -1):
        far = plane + delta
        pl.when(jnp.logical_and(far >= 0, far < PLANES))(functools.partial(greet, delta))
    greet(0)
    for off in range(1, nf):
        pl.semaphore_signal(
            barrier, inc=1, device_id=(lax.rem(b + off, nf), me), device_id_type=MESH
        )

    load_w.start()
    load_trig.start()
    for th in range(chunks):
        load_x(th).start()
    load_god.start()
    load_own.start()

    load_w.wait()
    load_trig.wait()
    weights = jnp.broadcast_to(w_ref[...], (length, length)).T * (1.0 / math.sqrt(length))
    odd = lax.rem(lax.broadcasted_iota(jnp.int32, (length // 2, length), 1), 2) == 1
    cosine, sine = (
        weights * jnp.concatenate([part, jnp.where(odd, -part, part)], axis=0)
        for part in (trig_ref[0], trig_ref[1])
    )
    matrix = jnp.concatenate(
        [jnp.concatenate([cosine, -sine], axis=1), jnp.concatenate([sine, cosine], axis=1)], axis=0
    )
    high = matrix.astype(jnp.bfloat16)
    low = (matrix - high.astype(jnp.float32)).astype(jnp.bfloat16)

    load(4, x_ref, x_ref).wait()
    for th in range(chunks):
        xf[th] = x_ref[th].astype(jnp.float32).reshape(rows * step, length)
    for th in range(chunks):
        parts = []
        for t in range(ch_out):
            re = xf[th, pl.ds(2 * t, rows, stride=step), :]
            im = xf[th, pl.ds(2 * t + 1, rows, stride=step), :]
            parts.append(jnp.concatenate([re, im], axis=1).astype(jnp.bfloat16))
        flat = jnp.concatenate(parts, axis=0)
        spectra = jnp.dot(flat, high, preferred_element_type=jnp.float32) + jnp.dot(
            flat, low, preferred_element_type=jnp.float32
        )
        for p in range(2):
            blocks = [
                spectra[i * rows : (i + 1) * rows, p * LANES : (p + 1) * LANES]
                for i in range(ch_out)
            ]
            blocks = deal_blocks(blocks, AVG)
            for k in range(ch_out):
                send1[k, th, :, p * LANES : (p + 1) * LANES] = blocks[k].astype(jnp.bfloat16)

    def whole(ref, sem):
        return pltpu.make_async_copy(ref, ref, sem.at[0])

    def first_copy(d, mine):
        return pltpu.make_async_remote_copy(
            src_ref=send1.at[d // spread],
            dst_ref=held.at[mine],
            send_sem=ssem1.at[d],
            recv_sem=rsem1.at[0],
            device_id=(b, d),
            device_id_type=MESH,
        )

    def tell(distance, delta):
        pl.semaphore_signal(
            hop_sem.at[2 * (distance - 2) + (delta < 0)], inc=1,
            device_id=(b, mate(-delta, 0)), device_id_type=MESH,
        )

    def hear(distance, delta):
        pl.semaphore_wait(hop_sem.at[2 * (distance - 2) + (delta < 0)], 1)

    def targets(at, entry):
        to = entry[0] if 2 * at < PLANES else PLANES - 1 - entry[0]
        return [mate(to - at, r) for r in range(entry[1], lanes, 2) if to != at or r]

    def is_send(entry):
        return isinstance(entry, tuple) and entry[0] != "tell"

    def each_role(run):
        for at in range(PLANES):
            inner = 0 < at < PLANES - 1
            for half in range(2):
                pl.when(jnp.logical_and(plane == at, lax.rem(b, 2) == half))(
                    functools.partial(run, at, inner, PLANS[at][half])
                )

    def send_first(at, inner, plan):
        up = 1 if 2 * at < PLANES else -1
        pl.semaphore_wait(barrier, (3 if inner else 2) * lanes - 1 + nf - 1)
        if inner:
            tell(2, up)
            tell(2, -up)
        for entry in plan:
            if entry == "h2":
                hear(2, up)
                if inner:
                    tell(3, up)
            elif entry == "h3":
                hear(3, up)
            elif entry == "wait":
                pl.semaphore_wait(twin_sem, 1)
            elif is_send(entry):
                for d in targets(at, entry):
                    first_copy(d, me).start()
            else:
                for sent in list(filter(is_send, plan))[: entry[1]]:
                    for d in targets(at, sent):
                        first_copy(d, me).wait_send()
                pl.semaphore_signal(
                    twin_sem, inc=1, device_id=(b + 1 - 2 * lax.rem(b, 2), me), device_id_type=MESH
                )

    each_role(send_first)

    for off in range(1, nf):
        pl.semaphore_signal(
            row_sem, inc=1, device_id=(lax.rem(b + off, nf), me), device_id_type=MESH
        )
    held[me] = send1[me // spread]

    load_god.wait()
    load_own.wait()

    def find_dev(g, carry):
        def body(s, acc):
            return jnp.where(god_ref[s] == g, s, acc)

        dev_of[g] = lax.fori_loop(0, ns, body, jnp.int32(0), unroll=min(ns, 8))
        return carry

    lax.fori_loop(0, ns, find_dev, 0)
    quarter = lax.rem(me, spread)

    def find_col(i, carry):
        g1 = quarter * ch_out + i // ns
        o = lax.rem(i, ns)

        def body(g2, acc):
            return jnp.where(own_ref[g1, g2] == o, dev_of[g2], acc)

        table[i] = lax.fori_loop(0, ns, body, jnp.int32(0), unroll=min(ns, 8))
        return carry

    lax.fori_loop(0, ch_out * ns, find_col, 0)
    pl.semaphore_wait(row_sem, nf - 1)

    channel = b * ch_out + me // spread
    first_row = quarter * fl_count

    def second_copy(fl, o):
        return pltpu.make_async_remote_copy(
            src_ref=send2.at[fl * ns + o],
            dst_ref=out_ref.at[:, channel],
            send_sem=ssem2.at[0],
            recv_sem=rsem2.at[0],
            device_id=(first_row + fl, o),
            device_id_type=MESH,
        )

    def unless_mine(fl, o, run):
        mine = jnp.logical_and(first_row + fl == b, o == me)
        pl.when(jnp.logical_not(mine))(run)

    per_tile = LANES // rows
    sub = rows // per_tile
    span = rpf * rows
    wide = min(2 * per_tile, ns)
    cols = wide * rows

    whole(held.at[: ns - 1], rsem1).wait()

    pair = 2 - fl_count % 2
    block_rows = 2 * span

    def correlate(f0):
        for u in range(pair):
            top = u * block_rows
            for g in range(rpf):
                x = held[dev_of[(first_row + f0 + u) * rpf + g]]
                at = top + g * rows
                for th in range(chunks):
                    left[th, at : at + rows, :] = x[th]
                    left[th, at + span : at + span + rows, :LANES] = x[th, :, LANES:]
                    left[th, at + span : at + span + rows, LANES:] = -x[th, :, :LANES]
        for c in range(ns // wide):
            for u in range(pair):
                block = sum(
                    lax.dot_general(
                        left[th, u * block_rows : (u + 1) * block_rows],
                        held[c * wide : (c + 1) * wide, th].reshape(cols, 2 * LANES),
                        (((1,), (1,)), ((), ())),
                        preferred_element_type=jnp.float32,
                    )
                    for th in range(chunks)
                ) * (1.0 / (AVG * spec))
                for h in range(cols // LANES):
                    vis[h, u * block_rows : (u + 1) * block_rows] = block[:, h * LANES : (h + 1) * LANES]
            for h in range(cols // LANES):
                blocks = [
                    vis[h, pl.ds(q, pair * block_rows // per_tile, stride=per_tile), :]
                    for q in range(per_tile)
                ]
                blocks = deal_blocks(blocks, rows)
                for s in range(per_tile):
                    whole = pltpu.roll(blocks[s], LANES - s * rows, 1) if s else blocks[s]
                    shaped = whole.reshape(pair, 2 * rpf, sub, LANES)
                    for u in range(pair):
                        tiles[f0 + u, c * wide + h * per_tile + s] = shaped[u]

    def build(fl, o):
        for g in range(rpf):
            source = table[(fl * rpf + g) * ns + o]
            for p in range(2):
                mixed[fl, o, p, pl.ds(g, sub, stride=rpf), :] = tiles[fl, source, p * rpf + g]
        for p in range(2):
            for r in range(sub):
                send2[fl * ns + o, p, :, r * LANES : (r + 1) * LANES] = mixed[
                    fl, o, p, r * rpf : (r + 1) * rpf, :
                ].astype(jnp.bfloat16)
        unless_mine(fl, o, lambda: second_copy(fl, o).start())

    for f0 in range(0, fl_count, pair):
        correlate(f0)

        def build_owner(o, carry):
            for u in range(pair):
                build(f0 + u, o)
            return carry

        lax.fori_loop(0, ns, build_owner, 0, unroll=min(ns, 8))

    own_here = quarter == b // fl_count

    @pl.when(own_here)
    def _():
        own = pltpu.make_async_copy(
            send2.at[lax.rem(b, fl_count) * ns + me], out_ref.at[:, channel], lsem.at[0]
        )
        own.start()
        own.wait()

    def end_first(at, inner, plan):
        done = sum(entry[1] for entry in plan if not is_send(entry) and entry[0] == "tell")
        for entry in list(filter(is_send, plan))[done:]:
            for d in targets(at, entry):
                first_copy(d, me).wait_send()

    each_role(end_first)

    def end_second(count):
        whole(send2.at[:count], ssem2).wait()
        whole(out_ref.at[:, :count], rsem2).wait()

    pl.when(own_here)(lambda: end_second(nf * ch_out - 1))
    pl.when(jnp.logical_not(own_here))(lambda: end_second(nf * ch_out))


def shards(nf, ns, samples, window, group_of_device, owner_map):
    _, rows, spec, _, length = samples.shape
    ch_out = length // AVG
    rpf = ns // nf
    fl_count = ch_out // rpf
    per_tile = LANES // rows
    sub = rows // per_tile
    chunks = spec // ch_out
    index = np.arange(length)
    theta = (index[: length // 2, None] * index[None, :] % length) * (2.0 * math.pi / length)
    trig = jnp.asarray(np.stack([np.cos(theta), np.sin(theta)]), jnp.float32)
    x = samples.reshape(rows, spec * 2, length)
    hbm = pl.BlockSpec(memory_space=pltpu.HBM)
    out = pl.pallas_call(
        functools.partial(kernel, nf, ns, rows, spec),
        out_shape=pltpu.VMEM((2, nf * ch_out, rpf, sub * LANES), jnp.bfloat16),
        in_specs=[hbm] * 5,
        out_specs=pl.BlockSpec(memory_space=OUT_SPACE),
        scratch_shapes=[
            pltpu.VMEM((chunks, rows, 2 * ch_out, length), jnp.bfloat16),
            pltpu.VMEM((1, length), jnp.float32),
            pltpu.VMEM((2, length // 2, length), jnp.float32),
            pltpu.SMEM((ns,), jnp.int32),
            pltpu.SMEM((ns, ns), jnp.int32),
            pltpu.VMEM((chunks, rows * 2 * ch_out, length), jnp.float32),
            pltpu.VMEM((ch_out, chunks, rows, 2 * LANES), jnp.bfloat16),
            pltpu.VMEM((ns, chunks, rows, 2 * LANES), jnp.bfloat16),
            pltpu.VMEM((chunks, 4 * rpf * rows, 2 * LANES), jnp.bfloat16),
            pltpu.VMEM((2, 4 * rpf * rows, LANES), jnp.float32),
            pltpu.VMEM((fl_count, ns, 2 * rpf, sub, LANES), jnp.float32),
            pltpu.VMEM((fl_count, ns, 2, sub * rpf, LANES), jnp.float32),
            pltpu.VMEM((fl_count * ns, 2, rpf, sub * LANES), jnp.bfloat16),
            pltpu.SMEM((ns,), jnp.int32),
            pltpu.SMEM((ch_out * ns,), jnp.int32),
            pltpu.SemaphoreType.DMA((5,)),
            pltpu.SemaphoreType.REGULAR,
            pltpu.SemaphoreType.REGULAR((2 * (PLANES - 2),)),
            pltpu.SemaphoreType.REGULAR,
            pltpu.SemaphoreType.DMA((ns,)),
            pltpu.SemaphoreType.DMA((1,)),
            pltpu.SemaphoreType.DMA((1,)),
            pltpu.SemaphoreType.DMA((1,)),
        ],
        compiler_params=pltpu.CompilerParams(
            collective_id=0, has_side_effects=True, vmem_limit_bytes=60 * 1024 * 1024
        ),
    )(x, window.reshape(1, length), trig, group_of_device, owner_map)
    return out[:, :, None]


def solution(mesh):
    return jax.shard_map(
        functools.partial(shards, mesh.shape["freq"], mesh.shape["stn"]),
        mesh=mesh,
        in_specs=(P("freq", "stn", None, None, None), P(), P(), P()),
        out_specs=P(None, None, "stn", "freq", None),
        check_vma=False,
    )
```

```python
import functools
import math

import jax
import jax.numpy as jnp
import numpy as np
from jax import lax
from jax.experimental import pallas as pl
from jax.experimental.pallas import tpu as pltpu
from jax.sharding import PartitionSpec as P

AVG = 16
LANES = 128
PLANES = 4
PLANS = (
    (
        ((1, 0), 'h2', (2, 0), 'h3', (3, 0), (3, 1), (1, 1), (2, 1), (0, 1), (0, 0), ('tell', 3)),
        ((1, 0), 'h2', 'h3', 'wait', (1, 1), (2, 0), (3, 0), (3, 1), (2, 1), (0, 0), (0, 1)),
    ),
    (
        ((2, 1), 'h2', (3, 0), (3, 1), (2, 0), (0, 0), (1, 1), (0, 1), (1, 0), ('tell', 3)),
        ((2, 1), 'h2', 'wait', (3, 1), (3, 0), (2, 0), (0, 0), (0, 1), (1, 1), (1, 0)),
    ),
    (
        ((2, 1), 'h2', (3, 1), (3, 0), (2, 0), (0, 0), (0, 1), (1, 1), (1, 0)),
        ((2, 1), 'h2', (3, 1), (3, 0), (2, 0), (0, 0), (1, 1), (0, 1), (1, 0)),
    ),
    (
        ((1, 0), 'h2', (2, 0), 'h3', (3, 0), (3, 1), (1, 1), (2, 1), (0, 1), (0, 0)),
        ((1, 0), 'h2', (2, 0), 'h3', (3, 0), (3, 1), (1, 1), (2, 1), (0, 1), (0, 0)),
    ),
)
MESH = pl.DeviceIdType.MESH
OUT_SPACE = pltpu.VMEM


def deal_blocks(blocks, width):
    count = len(blocks)
    lane = lax.broadcasted_iota(jnp.int32, blocks[0].shape, 1) // width
    turned = [pltpu.roll(x, i * width, 1) if i else x for i, x in enumerate(blocks)]
    dealt = [turned[-k % count] for k in range(count)]
    step = 1
    while step < count:
        upper = (lane // step) % 2 == 1
        dealt = [jnp.where(upper, dealt[(k - step) % count], dealt[k]) for k in range(count)]
        step *= 2
    return dealt


def kernel(
    nf, ns, rows, spec,
    x_hbm, w_hbm, trig_hbm, god_hbm, own_hbm,
    out_ref,
    x_ref, w_ref, trig_ref, god_ref, own_ref,
    xf, send1, held, left, vis, tiles, mixed, send2, dev_of, table,
    lsem, row_sem, hop_sem, twin_sem, ssem1, rsem1, ssem2, rsem2,
):
    length = LANES
    ch_out = length // AVG
    spread = ns // ch_out
    rpf = ns // nf
    fl_count = ch_out // rpf
    chunks = spec // ch_out
    step = 2 * ch_out
    lanes = ns // PLANES
    b = lax.axis_index("freq")
    me = lax.axis_index("stn")
    plane = me // lanes
    lane = lax.rem(me, lanes)

    def load(n, src, dst):
        return pltpu.make_async_copy(src, dst, lsem.at[n])

    def load_x(th):
        return load(4, x_hbm.at[:, th * step : (th + 1) * step, :], x_ref.at[th])

    load_w = load(0, w_hbm, w_ref)
    load_trig = load(1, trig_hbm, trig_ref)
    load_god = load(2, god_hbm, god_ref)
    load_own = load(3, own_hbm, own_ref)

    barrier = pltpu.get_barrier_semaphore()
    def mate(delta, r):
        return (plane + delta) * lanes + lax.rem(lane + r, lanes)

    def greet(delta):
        for r in range(lanes):
            if delta or r:
                pl.semaphore_signal(
                    barrier, inc=1, device_id=(b, mate(delta, r)), device_id_type=MESH
                )

    for delta in (1, -1):
        far = plane + delta
        pl.when(jnp.logical_and(far >= 0, far < PLANES))(functools.partial(greet, delta))
    greet(0)
    for off in range(1, nf):
        pl.semaphore_signal(
            barrier, inc=1, device_id=(lax.rem(b + off, nf), me), device_id_type=MESH
        )

    load_w.start()
    load_trig.start()
    for th in range(chunks):
        load_x(th).start()

    load_w.wait()
    load_trig.wait()
    weights = jnp.broadcast_to(w_ref[...], (length, length)).T * (1.0 / math.sqrt(length))
    odd = lax.rem(lax.broadcasted_iota(jnp.int32, (length // 2, length), 1), 2) == 1
    cosine, sine = (
        weights * jnp.concatenate([part, jnp.where(odd, -part, part)], axis=0)
        for part in (trig_ref[0], trig_ref[1])
    )
    matrix = jnp.concatenate(
        [jnp.concatenate([cosine, -sine], axis=1), jnp.concatenate([sine, cosine], axis=1)], axis=0
    )
    high = matrix.astype(jnp.bfloat16)
    low = (matrix - high.astype(jnp.float32)).astype(jnp.bfloat16)

    load(4, x_ref, x_ref).wait()
    for th in range(chunks):
        xf[th] = x_ref[th].astype(jnp.float32).reshape(rows * step, length)
    for th in range(chunks):
        parts = []
        for t in range(ch_out):
            re = xf[th, pl.ds(2 * t, rows, stride=step), :]
            im = xf[th, pl.ds(2 * t + 1, rows, stride=step), :]
            parts.append(jnp.concatenate([re, im], axis=1).astype(jnp.bfloat16))
        flat = jnp.concatenate(parts, axis=0)
        spectra = jnp.dot(flat, high, preferred_element_type=jnp.float32) + jnp.dot(
            flat, low, preferred_element_type=jnp.float32
        )
        for p in range(2):
            blocks = [
                spectra[i * rows : (i + 1) * rows, p * LANES : (p + 1) * LANES]
                for i in range(ch_out)
            ]
            blocks = deal_blocks(blocks, AVG)
            for k in range(ch_out):
                send1[k, th, :, p * LANES : (p + 1) * LANES] = blocks[k].astype(jnp.bfloat16)

    def whole(ref, sem):
        return pltpu.make_async_copy(ref, ref, sem.at[0])

    def first_copy(d, mine):
        return pltpu.make_async_remote_copy(
            src_ref=send1.at[d // spread],
            dst_ref=held.at[mine],
            send_sem=ssem1.at[d],
            recv_sem=rsem1.at[0],
            device_id=(b, d),
            device_id_type=MESH,
        )

    def tell(distance, delta):
        pl.semaphore_signal(
            hop_sem.at[2 * (distance - 2) + (delta < 0)], inc=1,
            device_id=(b, mate(-delta, 0)), device_id_type=MESH,
        )

    def hear(distance, delta):
        pl.semaphore_wait(hop_sem.at[2 * (distance - 2) + (delta < 0)], 1)

    def targets(at, entry):
        to = entry[0] if 2 * at < PLANES else PLANES - 1 - entry[0]
        return [mate(to - at, r) for r in range(entry[1], lanes, 2) if to != at or r]

    def is_send(entry):
        return isinstance(entry, tuple) and entry[0] != "tell"

    def each_role(run):
        for at in range(PLANES):
            inner = 0 < at < PLANES - 1
            for half in range(2):
                pl.when(jnp.logical_and(plane == at, lax.rem(b, 2) == half))(
                    functools.partial(run, at, inner, PLANS[at][half])
                )

    def send_first(at, inner, plan):
        up = 1 if 2 * at < PLANES else -1
        pl.semaphore_wait(barrier, (3 if inner else 2) * lanes - 1 + nf - 1)
        if inner:
            tell(2, up)
            tell(2, -up)
        for entry in plan:
            if entry == "h2":
                hear(2, up)
                if inner:
                    tell(3, up)
            elif entry == "h3":
                hear(3, up)
            elif entry == "wait":
                pl.semaphore_wait(twin_sem, 1)
            elif is_send(entry):
                for d in targets(at, entry):
                    first_copy(d, me).start()
            else:
                for sent in list(filter(is_send, plan))[: entry[1]]:
                    for d in targets(at, sent):
                        first_copy(d, me).wait_send()
                pl.semaphore_signal(
                    twin_sem, inc=1, device_id=(b + 1 - 2 * lax.rem(b, 2), me), device_id_type=MESH
                )

    each_role(send_first)
    load_god.start()
    load_own.start()

    for off in range(1, nf):
        pl.semaphore_signal(
            row_sem, inc=1, device_id=(lax.rem(b + off, nf), me), device_id_type=MESH
        )
    held[me] = send1[me // spread]

    load_god.wait()
    load_own.wait()

    def find_dev(g, carry):
        def body(s, acc):
            return jnp.where(god_ref[s] == g, s, acc)

        dev_of[g] = lax.fori_loop(0, ns, body, jnp.int32(0), unroll=min(ns, 8))
        return carry

    lax.fori_loop(0, ns, find_dev, 0)
    quarter = lax.rem(me, spread)

    def find_col(i, carry):
        g1 = quarter * ch_out + i // ns
        o = lax.rem(i, ns)

        def body(g2, acc):
            return jnp.where(own_ref[g1, g2] == o, dev_of[g2], acc)

        table[i] = lax.fori_loop(0, ns, body, jnp.int32(0), unroll=min(ns, 8))
        return carry

    lax.fori_loop(0, ch_out * ns, find_col, 0)
    pl.semaphore_wait(row_sem, nf - 1)

    channel = b * ch_out + me // spread
    first_row = quarter * fl_count

    def second_copy(fl, o):
        return pltpu.make_async_remote_copy(
            src_ref=send2.at[fl * ns + o],
            dst_ref=out_ref.at[:, channel],
            send_sem=ssem2.at[0],
            recv_sem=rsem2.at[0],
            device_id=(first_row + fl, o),
            device_id_type=MESH,
        )

    def unless_mine(fl, o, run):
        mine = jnp.logical_and(first_row + fl == b, o == me)
        pl.when(jnp.logical_not(mine))(run)

    per_tile = LANES // rows
    sub = rows // per_tile
    span = rpf * rows
    wide = min(2 * per_tile, ns)
    cols = wide * rows

    whole(held.at[: ns - 1], rsem1).wait()

    pair = 2 - fl_count % 2
    block_rows = 2 * span

    def correlate(f0):
        for u in range(pair):
            top = u * block_rows
            for g in range(rpf):
                x = held[dev_of[(first_row + f0 + u) * rpf + g]]
                at = top + g * rows
                for th in range(chunks):
                    left[th, at : at + rows, :] = x[th]
                    left[th, at + span : at + span + rows, :LANES] = x[th, :, LANES:]
                    left[th, at + span : at + span + rows, LANES:] = -x[th, :, :LANES]
        for c in range(ns // wide):
            for u in range(pair):
                block = sum(
                    lax.dot_general(
                        left[th, u * block_rows : (u + 1) * block_rows],
                        held[c * wide : (c + 1) * wide, th].reshape(cols, 2 * LANES),
                        (((1,), (1,)), ((), ())),
                        preferred_element_type=jnp.float32,
                    )
                    for th in range(chunks)
                ) * (1.0 / (AVG * spec))
                for h in range(cols // LANES):
                    vis[h, u * block_rows : (u + 1) * block_rows] = block[:, h * LANES : (h + 1) * LANES]
            for h in range(cols // LANES):
                blocks = [
                    vis[h, pl.ds(q, pair * block_rows // per_tile, stride=per_tile), :]
                    for q in range(per_tile)
                ]
                blocks = deal_blocks(blocks, rows)
                for s in range(per_tile):
                    whole = pltpu.roll(blocks[s], LANES - s * rows, 1) if s else blocks[s]
                    shaped = whole.reshape(pair, 2 * rpf, sub, LANES)
                    for u in range(pair):
                        tiles[f0 + u, c * wide + h * per_tile + s] = shaped[u]

    def build(fl, o):
        for g in range(rpf):
            source = table[(fl * rpf + g) * ns + o]
            for p in range(2):
                mixed[fl, o, p, pl.ds(g, sub, stride=rpf), :] = tiles[fl, source, p * rpf + g]
        for p in range(2):
            for r in range(sub):
                send2[fl * ns + o, p, :, r * LANES : (r + 1) * LANES] = mixed[
                    fl, o, p, r * rpf : (r + 1) * rpf, :
                ].astype(jnp.bfloat16)
        unless_mine(fl, o, lambda: second_copy(fl, o).start())

    for f0 in range(0, fl_count, pair):
        correlate(f0)

        def build_owner(o, carry):
            for u in range(pair):
                build(f0 + u, o)
            return carry

        lax.fori_loop(0, ns, build_owner, 0, unroll=min(ns, 8))

    own_here = quarter == b // fl_count

    @pl.when(own_here)
    def _():
        own = pltpu.make_async_copy(
            send2.at[lax.rem(b, fl_count) * ns + me], out_ref.at[:, channel], lsem.at[0]
        )
        own.start()
        own.wait()

    def end_first(at, inner, plan):
        done = sum(entry[1] for entry in plan if not is_send(entry) and entry[0] == "tell")
        for entry in list(filter(is_send, plan))[done:]:
            for d in targets(at, entry):
                first_copy(d, me).wait_send()

    each_role(end_first)

    def end_second(count):
        whole(send2.at[:count], ssem2).wait()
        whole(out_ref.at[:, :count], rsem2).wait()

    pl.when(own_here)(lambda: end_second(nf * ch_out - 1))
    pl.when(jnp.logical_not(own_here))(lambda: end_second(nf * ch_out))


def shards(nf, ns, samples, window, group_of_device, owner_map):
    _, rows, spec, _, length = samples.shape
    ch_out = length // AVG
    rpf = ns // nf
    fl_count = ch_out // rpf
    per_tile = LANES // rows
    sub = rows // per_tile
    chunks = spec // ch_out
    index = np.arange(length)
    theta = (index[: length // 2, None] * index[None, :] % length) * (2.0 * math.pi / length)
    trig = jnp.asarray(np.stack([np.cos(theta), np.sin(theta)]), jnp.float32)
    x = samples.reshape(rows, spec * 2, length)
    hbm = pl.BlockSpec(memory_space=pltpu.HBM)
    out = pl.pallas_call(
        functools.partial(kernel, nf, ns, rows, spec),
        out_shape=pltpu.VMEM((2, nf * ch_out, rpf, sub * LANES), jnp.bfloat16),
        in_specs=[hbm] * 5,
        out_specs=pl.BlockSpec(memory_space=OUT_SPACE),
        scratch_shapes=[
            pltpu.VMEM((chunks, rows, 2 * ch_out, length), jnp.bfloat16),
            pltpu.VMEM((1, length), jnp.float32),
            pltpu.VMEM((2, length // 2, length), jnp.float32),
            pltpu.SMEM((ns,), jnp.int32),
            pltpu.SMEM((ns, ns), jnp.int32),
            pltpu.VMEM((chunks, rows * 2 * ch_out, length), jnp.float32),
            pltpu.VMEM((ch_out, chunks, rows, 2 * LANES), jnp.bfloat16),
            pltpu.VMEM((ns, chunks, rows, 2 * LANES), jnp.bfloat16),
            pltpu.VMEM((chunks, 4 * rpf * rows, 2 * LANES), jnp.bfloat16),
            pltpu.VMEM((2, 4 * rpf * rows, LANES), jnp.float32),
            pltpu.VMEM((fl_count, ns, 2 * rpf, sub, LANES), jnp.float32),
            pltpu.VMEM((fl_count, ns, 2, sub * rpf, LANES), jnp.float32),
            pltpu.VMEM((fl_count * ns, 2, rpf, sub * LANES), jnp.bfloat16),
            pltpu.SMEM((ns,), jnp.int32),
            pltpu.SMEM((ch_out * ns,), jnp.int32),
            pltpu.SemaphoreType.DMA((5,)),
            pltpu.SemaphoreType.REGULAR,
            pltpu.SemaphoreType.REGULAR((2 * (PLANES - 2),)),
            pltpu.SemaphoreType.REGULAR,
            pltpu.SemaphoreType.DMA((ns,)),
            pltpu.SemaphoreType.DMA((1,)),
            pltpu.SemaphoreType.DMA((1,)),
            pltpu.SemaphoreType.DMA((1,)),
        ],
        compiler_params=pltpu.CompilerParams(
            collective_id=0, has_side_effects=True, vmem_limit_bytes=60 * 1024 * 1024
        ),
    )(x, window.reshape(1, length), trig, group_of_device, owner_map)
    return out[:, :, None]


def solution(mesh):
    return jax.shard_map(
        functools.partial(shards, mesh.shape["freq"], mesh.shape["stn"]),
        mesh=mesh,
        in_specs=(P("freq", "stn", None, None, None), P(), P(), P()),
        out_specs=P(None, None, "stn", "freq", None),
        check_vma=False,
    )
```
